32 devices in a mesh: row: 8 (over z, x), col: 4 (over y, core).
Axes of the slice: x: 2, y: 2, z: 4, core: 2. Of those that a mesh axis runs over, the one named last changes fastest.
Arguments:
- left: bfloat16 [128, 4096], P('col', 'row'), may hold values from -6 to 6
- right: bfloat16 [128, 4096], P('row', 'col'), may hold values from -6 to 6
- pair_in: bfloat16 [128, 128, 128], P('row', 'col'), may hold values from -6 to 6
- pair_cot: bfloat16 [128, 128, 128], P('row', 'col'), may hold values from -6 to 6
- ln_gain: float32 [128], replicated, may hold values from 0.25 to 1.75
- out_weight: bfloat16 [1024, 128], replicated, may hold values from -2 to 2
- out_bias: float32 [128], replicated, may hold values from -3 to 3
- trans_up: bfloat16 [128, 512], replicated, may hold values from -0.5 to 0.5
- trans_down: bfloat16 [512, 128], replicated, may hold values from -0.25 to 0.25
Outputs:
- pair_out: bfloat16 [128, 128, 128], P('row', 'col')
- grad_left: bfloat16 [128, 4096], P('col', 'row')
- grad_right: bfloat16 [128, 4096], P('row', 'col')
The draws below stay inside these ranges and needn't reach their ends.
All inputs are finite; a program needn't handle non-finite values.
Results may differ from the reference program's by a relative error of at most 0.01.
The reference program's roundings to bfloat16 on the way (of `outer`, `normed`, `hidden`, `d_hidden`, `d_middle` and `d_outer`) count: a program that leaves them out, or rounds other values in their place, can miss the bound.
Values may be sent and summed in bfloat16 or wider, within the bound.
A program may use at most 64 MiB of HBM per device.

```python
import jax
import jax.numpy as jnp
from jax import lax

C = 32
PAIR = 128
FFN = 512
SEQS = 128
CROP = 128
N_ROW = 8


def block_levels(stream_key, extent, split, least, top_value):
    def one(axis_at, shards_of):
        draws = jax.random.uniform(jax.random.fold_in(jax.random.fold_in(stream_key, 6), axis_at), (shards_of,), jnp.float32, least / len(split), top_value / len(split))
        return jnp.repeat(jnp.exp(draws), extent[axis_at] // shards_of).reshape((-1,) + (1,) * (len(extent) - axis_at - 1))

    level = one(*split[0])
    for cut in split[1:]:
        level = level * one(*cut)
    return level


def bell_draw(rng, extent, width, most, pieces=(), kind=jnp.bfloat16):
    entries = width * jax.random.normal(rng, extent, jnp.float32)
    if pieces:
        entries = entries * block_levels(rng, extent, pieces, -0.22, 0.18)
    return jnp.clip(entries, -most, most).astype(kind)


def setup_inputs(seed: int = 0) -> dict:
    splits = jax.random.split(jax.random.key(seed), 10)
    left = bell_draw(splits[0], (SEQS, CROP * C), 1.0, 6.0, ((0, 4), (1, 8)))
    right = bell_draw(splits[1], (SEQS, CROP * C), 1.0, 6.0, ((0, 8), (1, 4)))
    pair_in = bell_draw(splits[2], (CROP, CROP, PAIR), 1.0, 6.0, ((0, 8), (1, 4)))
    pair_cot = bell_draw(splits[3], (CROP, CROP, PAIR), 1.0, 6.0, ((0, 8), (1, 4)))
    ln_gain = jnp.clip(1.0 + 0.15 * jax.random.normal(splits[4], (PAIR,), jnp.float32), 0.25, 1.75)
    out_weight = bell_draw(splits[5], (C * C, PAIR), (C * C // SEQS) ** -0.5, 2.0)
    out_bias = bell_draw(splits[6], (PAIR,), 0.5, 3.0, (), jnp.float32)
    trans_up = bell_draw(splits[7], (PAIR, FFN), PAIR ** -0.5, 0.5)
    trans_down = bell_draw(splits[8], (FFN, PAIR), FFN ** -0.5, 0.25)
    return dict(left=left, right=right, pair_in=pair_in, pair_cot=pair_cot, ln_gain=ln_gain, out_weight=out_weight, out_bias=out_bias, trans_up=trans_up, trans_down=trans_down)


def pair_block(outer, pair_in, pair_cot, ln_gain, out_weight, out_bias, trans_up, trans_down):
    update = jnp.einsum('ijk,kd->ijd', outer.astype(jnp.float32), out_weight.astype(jnp.float32))
    middle = pair_in.astype(jnp.float32) + update + out_bias
    centre = lax.optimization_barrier(jnp.mean(middle, axis=-1, keepdims=True))
    centred = middle - centre
    spread = lax.optimization_barrier(jnp.mean(centred * centred, axis=-1, keepdims=True))
    inverse = lax.rsqrt(spread + 1e-05)
    normal_x = centred * inverse
    normed = (normal_x * ln_gain).astype(jnp.bfloat16)
    preact = jnp.einsum('ijk,kf->ijf', normed.astype(jnp.float32), trans_up.astype(jnp.float32))
    hidden = jnp.maximum(preact, 0.0).astype(jnp.bfloat16)
    down = jnp.einsum('ijf,fk->ijk', hidden.astype(jnp.float32), trans_down.astype(jnp.float32))
    pair_out = (middle + down).astype(jnp.bfloat16)
    cotangent = pair_cot.astype(jnp.float32)
    back = jnp.einsum('ijk,fk->ijf', cotangent, trans_down.astype(jnp.float32))
    d_hidden = jnp.where(preact > 0.0, back, 0.0).astype(jnp.bfloat16)
    d_normed = jnp.einsum('ijf,kf->ijk', d_hidden.astype(jnp.float32), trans_up.astype(jnp.float32))
    scaled = d_normed * ln_gain
    d_middle = cotangent + inverse * (scaled - lax.optimization_barrier(jnp.mean(scaled, axis=-1, keepdims=True)) - normal_x * lax.optimization_barrier(jnp.mean(scaled * normal_x, axis=-1, keepdims=True)))
    d_middle = d_middle.astype(jnp.bfloat16)
    d_outer = jnp.einsum('ijk,ck->ijc', d_middle.astype(jnp.float32), out_weight.astype(jnp.float32))
    return (pair_out, d_outer.astype(jnp.bfloat16))

def reference(left, right, pair_in, pair_cot, ln_gain, out_weight, out_bias, trans_up, trans_down):
    crop = pair_in.shape[0]
    block = crop // N_ROW
    left_all = left.reshape(SEQS, crop, C).astype(jnp.float32)
    right_all = right.reshape(SEQS, crop, C).astype(jnp.float32)

    def step(carry, index):
        first = (index * block).astype(jnp.int32)
        left_rows = lax.dynamic_slice_in_dim(left_all, first, block, 1)
        pair_rows = lax.dynamic_slice_in_dim(pair_in, first, block, 0)
        cot_rows = lax.dynamic_slice_in_dim(pair_cot, first, block, 0)
        summed = jnp.einsum('sic,sje->ijce', left_rows, right_all)
        outer = (summed * (1.0 / SEQS)).astype(jnp.bfloat16).reshape(block, crop, C * C)
        pair_rows_out, d_outer = pair_block(outer, pair_rows, cot_rows, ln_gain, out_weight, out_bias, trans_up, trans_down)
        grad_tiles = d_outer.reshape(block, crop, C, C).astype(jnp.float32)
        left_grad = jnp.einsum('ijce,sje->sic', grad_tiles, right_all) * (1.0 / SEQS)
        carry = carry + jnp.einsum('ijce,sic->sje', grad_tiles, left_rows)
        return (carry, (pair_rows_out, left_grad.astype(jnp.bfloat16)))
    start_carry = jnp.zeros((SEQS, crop, C), jnp.float32)
    carry, stacked = lax.scan(step, start_carry, jnp.arange(N_ROW, dtype=jnp.int32))
    pair_out = stacked[0].reshape(crop, crop, pair_in.shape[2])
    grad_left = jnp.moveaxis(stacked[1], 0, 1).reshape(SEQS, crop * C)
    grad_right = (carry * (1.0 / SEQS)).astype(jnp.bfloat16).reshape(SEQS, crop * C)
    return (pair_out, grad_left, grad_right)
```

```python
import functools

import jax
import jax.numpy as jnp
from jax import lax
from jax.experimental import pallas as pl
from jax.experimental.pallas import tpu as pltpu
from jax.sharding import PartitionSpec as P

C = 32
LANES = 128
QUARTERS = LANES // C
CHUNK = 256
BF16 = jnp.bfloat16
F32 = jnp.float32
NN = (((1,), (0,)), ((), ()))
NT = (((1,), (1,)), ((), ()))


def mm(x, y, dims=NN):
    return lax.dot_general(x, y, dims, preferred_element_type=F32)


def swap_perm(major, minor):
    size = major * minor
    row = lax.broadcasted_iota(jnp.int32, (size, size), 0)
    column = lax.broadcasted_iota(jnp.int32, (size, size), 1)
    return jnp.where(column == (row % minor) * major + row // minor, 1.0, 0.0).astype(BF16)


def quarter_transpose(parts):
    turned = [x if p == 0 else pltpu.roll(x, p * C, 1) for p, x in enumerate(parts)]
    group = lax.broadcasted_iota(jnp.int32, parts[0].shape, 1) // C
    out = []
    for k in range(QUARTERS):
        y = turned[(QUARTERS - 1 - k) % QUARTERS]
        for q in range(QUARTERS - 1):
            y = jnp.where(group == q, turned[(q - k) % QUARTERS], y)
        out.append(y if k == 0 else pltpu.roll(y, LANES - k * C, 1))
    return out


def kernel(
    nrow, ncol, rows, cols,
    left_ref, right_ref, pin_ref, cot_ref, gain_ref, w_ref, bias_ref, up_ref, down_ref,
    out_ref, gl_ref, gr_ref,
    left_v, right_v, pin_v, cot_v, w_v, up_v, down_v,
    a_buf, b_buf, perm_v, permt_v, pin_p, cot_p, back_v, a_p, a_pt, o_v, out_p, d_v,
    gr_send, gr_recv, gl_acc, gl_send, gl_recv,
    load_sem, a_send_sem, a_recv_sem, b_send_sem, b_recv_sem,
    gr_send_sem, gr_recv_sem, gl_send_sem, gl_recv_sem,
):
    me_r = lax.axis_index("row")
    me_c = lax.axis_index("col")
    nch = b_buf.shape[0]
    seqs = a_p.shape[0]
    scale = 1.0 / seqs
    loads = [
        pltpu.make_async_copy(src, dst, load_sem.at[n])
        for n, (src, dst) in enumerate(
            [
                (left_ref, left_v),
                (right_ref, right_v),
                (pin_ref, pin_v),
                (cot_ref, cot_v),
                (down_ref, down_v),
                (w_ref, w_v),
                (up_ref, up_v),
            ]
        )
    ]
    for load in loads:
        load.start()

    def row_peer(d):
        return lax.rem(me_r + d, nrow)

    def col_peer(d):
        return lax.rem(me_c + d, ncol)

    barrier = pltpu.get_barrier_semaphore()
    for d in range(1, nrow):
        pl.semaphore_signal(
            barrier, inc=1, device_id=(row_peer(d), me_c), device_id_type=pl.DeviceIdType.MESH
        )
    for d in range(1, ncol):
        pl.semaphore_signal(
            barrier, inc=1, device_id=(me_r, col_peer(d)), device_id_type=pl.DeviceIdType.MESH
        )
    loads[0].wait()
    loads[1].wait()
    a_buf[me_c] = left_v[...]
    for k in range(nch):
        b_buf[k, me_r] = right_v[:, k * CHUNK:(k + 1) * CHUNK]
    pl.semaphore_wait(barrier, nrow + ncol - 2)

    def a_copy(d):
        to = col_peer(d)
        return pltpu.make_async_remote_copy(
            src_ref=left_v, dst_ref=a_buf.at[me_c],
            send_sem=a_send_sem.at[d], recv_sem=a_recv_sem.at[me_c],
            device_id=(me_r, to), device_id_type=pl.DeviceIdType.MESH,
        )

    def b_copy(k, d):
        to = row_peer(d)
        return pltpu.make_async_remote_copy(
            src_ref=right_v.at[:, k * CHUNK:(k + 1) * CHUNK], dst_ref=b_buf.at[k, me_r],
            send_sem=b_send_sem.at[k, d], recv_sem=b_recv_sem.at[k, me_r],
            device_id=(to, me_c), device_id_type=pl.DeviceIdType.MESH,
        )

    def gr_copy(k, d):
        to = row_peer(d)
        return pltpu.make_async_remote_copy(
            src_ref=gr_send.at[k, to], dst_ref=gr_recv.at[k, me_r],
            send_sem=gr_send_sem.at[k, d], recv_sem=gr_recv_sem.at[k, me_r],
            device_id=(to, me_c), device_id_type=pl.DeviceIdType.MESH,
        )

    def gl_copy(d):
        to = col_peer(d)
        return pltpu.make_async_remote_copy(
            src_ref=gl_send.at[to], dst_ref=gl_recv.at[me_c],
            send_sem=gl_send_sem.at[d], recv_sem=gl_recv_sem.at[me_c],
            device_id=(me_r, to), device_id_type=pl.DeviceIdType.MESH,
        )

    def landed(buf, sem):
        pltpu.make_async_copy(buf, buf, sem).wait()

    sends = []

    def go(copy):
        copy.start()
        sends.append(copy)

    for d in range(1, ncol):
        go(a_copy(d))
    for k in range(nch):
        for d in range(1, nrow):
            go(b_copy(k, d))

    perm_v[...] = swap_perm(C, rows)
    permt_v[...] = swap_perm(rows, C)
    if cols == C:
        pair_perm, pair_permt = perm_v[...], permt_v[...]
    else:
        pair_perm, pair_permt = swap_perm(cols, rows), swap_perm(rows, cols)
    for load in loads[2:]:
        load.wait()
    pairs = rows * cols
    width = pin_v.shape[2]
    gain = gain_ref[...].reshape(1, width)
    bias = bias_ref[...].reshape(1, width)
    pin_p[...] = mm(pair_perm, pin_v[...].reshape(pairs, width)) + bias
    cot_p[...] = mm(pair_perm, cot_v[...].reshape(pairs, width)).astype(BF16)
    back_v[...] = mm(cot_p[...], down_v[...], NT)

    for d in range(1, ncol):
        src = col_peer(d)
        landed(a_buf.at[src], a_recv_sem.at[src])
    a_all = a_buf[...].reshape(seqs, rows * C)
    a_p[...] = mm(a_all, permt_v[...]).astype(BF16)
    a_pt[...] = (mm(perm_v[...], a_all, NT) * scale).astype(BF16)

    part = CHUNK // C * rows
    tiles = CHUNK // LANES
    blocks = C // QUARTERS
    for k in range(nch):
        for d in range(1, nrow):
            src = row_peer(d)
            landed(b_buf.at[k, src], b_recv_sem.at[k, src])
        b_k = b_buf[k].reshape(seqs, CHUNK)
        m = mm(a_pt[...], b_k)
        for t in range(tiles):
            for h in range(blocks):
                r = quarter_transpose(
                    [
                        m[(h * QUARTERS + q) * rows:(h * QUARTERS + q + 1) * rows, t * LANES:(t + 1) * LANES]
                        for q in range(QUARTERS)
                    ]
                )
                for q in range(QUARTERS):
                    j = t * QUARTERS + q
                    o_v[j * rows:(j + 1) * rows, h * LANES:(h + 1) * LANES] = r[q].astype(BF16)
        span = slice(k * part, (k + 1) * part)
        middle = pin_p[span, :] + mm(o_v[...], w_v[...])
        centred = middle - jnp.mean(middle, axis=-1, keepdims=True)
        inverse = lax.rsqrt(jnp.mean(centred * centred, axis=-1, keepdims=True) + 1e-05)
        xhat = centred * inverse
        normed = (xhat * gain).astype(BF16)
        preact = mm(normed, up_v[...])
        hidden = jnp.maximum(preact, 0.0).astype(BF16)
        d_hidden = jnp.where(preact > 0.0, back_v[span, :], 0.0).astype(BF16)
        d_normed = mm(d_hidden, up_v[...], NT)
        scaled = d_normed * gain
        d_middle = cot_p[span, :].astype(F32) + inverse * (
            scaled
            - jnp.mean(scaled, axis=-1, keepdims=True)
            - xhat * jnp.mean(scaled * xhat, axis=-1, keepdims=True)
        )
        d_outer = mm(d_middle.astype(BF16), w_v[...], NT)
        for t in range(tiles):
            for h in range(blocks):
                r = quarter_transpose(
                    [
                        d_outer[(t * QUARTERS + q) * rows:(t * QUARTERS + q + 1) * rows, h * LANES:(h + 1) * LANES]
                        for q in range(QUARTERS)
                    ]
                )
                for q in range(QUARTERS):
                    c = h * QUARTERS + q
                    d_v[c * rows:(c + 1) * rows, t * LANES:(t + 1) * LANES] = r[q].astype(BF16)
        gr_send[k] = mm(a_p[...], d_v[...]).astype(BF16).reshape(gr_send.shape[1:])
        for d in range(1, nrow):
            go(gr_copy(k, d))
        gl = mm(b_k, d_v[...], NT)
        if k == 0:
            gl_acc[...] = gl
        elif k < nch - 1:
            gl_acc[...] += gl
        else:
            gl_send[...] = (gl_acc[...] + gl).astype(BF16).reshape(gl_send.shape)
            for d in range(1, ncol):
                go(gl_copy(d))
        down = mm(hidden, down_v[...])
        out_p[span, :] = (middle + down).astype(BF16)

    out_ref[...] = mm(pair_permt, out_p[...]).astype(BF16).reshape(out_ref.shape)

    for k in range(nch):
        total = gr_send[k, me_r].astype(F32)
        for d in range(1, nrow):
            src = row_peer(d)
            landed(gr_recv.at[k, src], gr_recv_sem.at[k, src])
            total = total + gr_recv[k, src].astype(F32)
        gr_ref[:, k * CHUNK:(k + 1) * CHUNK] = (total * scale).astype(BF16)
    total = gl_send[me_c].astype(F32)
    for d in range(1, ncol):
        src = col_peer(d)
        landed(gl_recv.at[src], gl_recv_sem.at[src])
        total = total + gl_recv[src].astype(F32)
    gl_ref[...] = mm((total * scale).astype(BF16), perm_v[...]).astype(BF16)
    for copy in sends:
        copy.wait_send()


def on_device(nrow, ncol, left, right, pair_in, pair_cot, ln_gain, out_weight, out_bias, trans_up, trans_down):
    rows, cols, width = pair_in.shape
    ls, lw = left.shape
    rs, rw = right.shape
    seqs = ls * ncol
    ffn = trans_up.shape[1]
    pairs = rows * cols
    nch = rw // CHUNK
    dma = pltpu.SemaphoreType.DMA
    vm = pltpu.VMEM
    scratch = [
        vm((ls, lw), BF16), vm((rs, rw), BF16),
        vm((rows, cols, width), BF16), vm((rows, cols, width), BF16),
        vm(out_weight.shape, BF16), vm(trans_up.shape, BF16), vm(trans_down.shape, BF16),
        vm((ncol, ls, lw), BF16), vm((nch, nrow, rs, CHUNK), BF16),
        vm((lw, lw), BF16), vm((lw, lw), BF16),
        vm((pairs, width), F32), vm((pairs, width), BF16), vm((pairs, ffn), F32),
        vm((seqs, lw), BF16), vm((lw, seqs), BF16),
        vm((CHUNK // C * rows, C * C), BF16), vm((pairs, width), BF16), vm((lw, CHUNK), BF16),
        vm((nch, nrow, rs, CHUNK), BF16), vm((nch, nrow, rs, CHUNK), BF16),
        vm((seqs, lw), F32), vm((ncol, ls, lw), BF16), vm((ncol, ls, lw), BF16),
        dma((7,)), dma((ncol,)), dma((ncol,)), dma((nch, nrow)), dma((nch, nrow)),
        dma((nch, nrow)), dma((nch, nrow)), dma((ncol,)), dma((ncol,)),
    ]
    hbm = pl.BlockSpec(memory_space=pl.ANY)
    vmem = pl.BlockSpec(memory_space=pltpu.VMEM)
    return pl.pallas_call(
        functools.partial(kernel, nrow, ncol, rows, cols),
        out_shape=(
            jax.ShapeDtypeStruct(pair_in.shape, BF16),
            jax.ShapeDtypeStruct(left.shape, BF16),
            jax.ShapeDtypeStruct(right.shape, BF16),
        ),
        in_specs=[hbm, hbm, hbm, hbm, vmem, hbm, vmem, hbm, hbm],
        out_specs=(vmem, vmem, vmem),
        scratch_shapes=scratch,
        compiler_params=pltpu.CompilerParams(collective_id=0, has_side_effects=True),
    )(left, right, pair_in, pair_cot, ln_gain, out_weight, out_bias, trans_up, trans_down)


def solution(mesh):
    nrow, ncol = mesh.shape["row"], mesh.shape["col"]
    return jax.shard_map(
        functools.partial(on_device, nrow, ncol),
        mesh=mesh,
        in_specs=(
            P("col", "row"),
            P("row", "col"),
            P("row", "col", None),
            P("row", "col", None),
            P(),
            P(),
            P(),
            P(),
            P(),
        ),
        out_specs=(P("row", "col", None), P("col", "row"), P("row", "col")),
        check_vma=False,
    )
```

```python
import functools

import jax
import jax.numpy as jnp
from jax import lax
from jax.experimental import pallas as pl
from jax.experimental.pallas import tpu as pltpu
from jax.sharding import PartitionSpec as P

C = 32
LANES = 128
QUARTERS = LANES // C
CHUNK = 512
LIMIT = 16 * 1024 * 1024
BF16 = jnp.bfloat16
F32 = jnp.float32
NN = (((1,), (0,)), ((), ()))
NT = (((1,), (1,)), ((), ()))


def mm(x, y, dims=NN):
    return lax.dot_general(x, y, dims, preferred_element_type=F32)


def swap_perm(major, minor):
    size = major * minor
    row = lax.broadcasted_iota(jnp.int32, (size, size), 0)
    column = lax.broadcasted_iota(jnp.int32, (size, size), 1)
    return jnp.where(column == (row % minor) * major + row // minor, 1.0, 0.0).astype(BF16)


def quarter_transpose(parts):
    turned = [x if p == 0 else pltpu.roll(x, p * C, 1) for p, x in enumerate(parts)]
    group = lax.broadcasted_iota(jnp.int32, parts[0].shape, 1) // C
    out = []
    for k in range(QUARTERS):
        y = turned[(QUARTERS - 1 - k) % QUARTERS]
        for q in range(QUARTERS - 1):
            y = jnp.where(group == q, turned[(q - k) % QUARTERS], y)
        out.append(y if k == 0 else pltpu.roll(y, LANES - k * C, 1))
    return out


def kernel(
    nrow, ncol, rows, cols,
    left_ref, right_ref, pin_ref, cot_ref, gain_ref, w_ref, bias_ref, up_ref, down_ref,
    out_ref, gl_ref, gr_ref,
    left_v, right_v, pin_v, cot_v, w_v, up_v, down_v, gain_v, bias_v,
    a_buf, b_buf, perm_v, permt_v, pin_p, cot_p, back_v, a_p, a_pt, o_v, hid_v, d_v,
    gr_send, gr_recv, gl_acc, gl_send, gl_recv,
    load_sem, a_send_sem, a_recv_sem, b_send_sem, b_recv_sem,
    gr_send_sem, gr_recv_sem, gl_send_sem, gl_recv_sem,
):
    me_r = lax.axis_index("row")
    me_c = lax.axis_index("col")
    nch = b_buf.shape[0]
    seqs = a_p.shape[0]
    scale = 1.0 / seqs
    loads = [
        pltpu.make_async_copy(src, dst, load_sem.at[n])
        for n, (src, dst) in enumerate(
            [
                (left_ref, left_v),
                (right_ref, right_v),
                (pin_ref, pin_v),
                (cot_ref, cot_v),
                (down_ref, down_v),
                (w_ref, w_v),
                (up_ref, up_v),
                (gain_ref, gain_v),
                (bias_ref, bias_v),
            ]
        )
    ]
    for load in loads:
        load.start()

    def row_peer(d):
        return lax.rem(me_r + d, nrow)

    def col_peer(d):
        return lax.rem(me_c + d, ncol)

    barrier = pltpu.get_barrier_semaphore()
    for d in range(1, nrow):
        pl.semaphore_signal(
            barrier, inc=1, device_id=(row_peer(d), me_c), device_id_type=pl.DeviceIdType.MESH
        )
    for d in range(1, ncol):
        pl.semaphore_signal(
            barrier, inc=1, device_id=(me_r, col_peer(d)), device_id_type=pl.DeviceIdType.MESH
        )
    loads[0].wait()
    loads[1].wait()
    a_buf[me_c] = left_v[...]
    for k in range(nch):
        b_buf[k, me_r] = right_v[:, k * CHUNK:(k + 1) * CHUNK]
    pl.semaphore_wait(barrier, nrow + ncol - 2)

    def a_copy(d):
        to = col_peer(d)
        return pltpu.make_async_remote_copy(
            src_ref=left_v, dst_ref=a_buf.at[me_c],
            send_sem=a_send_sem.at[d], recv_sem=a_recv_sem.at[me_c],
            device_id=(me_r, to), device_id_type=pl.DeviceIdType.MESH,
        )

    def b_copy(k, d):
        to = row_peer(d)
        return pltpu.make_async_remote_copy(
            src_ref=right_v.at[:, k * CHUNK:(k + 1) * CHUNK], dst_ref=b_buf.at[k, me_r],
            send_sem=b_send_sem.at[k, d], recv_sem=b_recv_sem.at[k, me_r],
            device_id=(to, me_c), device_id_type=pl.DeviceIdType.MESH,
        )

    def gr_copy(k, d):
        to = row_peer(d)
        return pltpu.make_async_remote_copy(
            src_ref=gr_send.at[k, to], dst_ref=gr_recv.at[k, me_r],
            send_sem=gr_send_sem.at[k, d], recv_sem=gr_recv_sem.at[k, me_r],
            device_id=(to, me_c), device_id_type=pl.DeviceIdType.MESH,
        )

    def gl_copy(d):
        to = col_peer(d)
        return pltpu.make_async_remote_copy(
            src_ref=gl_send.at[to], dst_ref=gl_recv.at[me_c],
            send_sem=gl_send_sem.at[d], recv_sem=gl_recv_sem.at[me_c],
            device_id=(me_r, to), device_id_type=pl.DeviceIdType.MESH,
        )

    def landed(buf, sem):
        pltpu.make_async_copy(buf, buf, sem).wait()

    sends = []

    def go(copy):
        copy.start()
        sends.append(copy)

    for d in range(1, ncol):
        go(a_copy(d))
    for k in range(nch):
        for d in sorted(range(1, nrow), key=lambda d: -min(d, nrow - d)):
            go(b_copy(k, d))

    perm_v[...] = swap_perm(C, rows)
    permt_v[...] = swap_perm(rows, C)
    if cols == C:
        pair_perm, pair_permt = perm_v[...], permt_v[...]
    else:
        pair_perm, pair_permt = swap_perm(cols, rows), swap_perm(rows, cols)
    for load in loads[2:]:
        load.wait()
    pairs = rows * cols
    width = pin_v.shape[2]
    gain = gain_v[...].reshape(1, width)
    bias = bias_v[...].reshape(1, width)
    pin_p[...] = mm(pair_perm, pin_v[...].reshape(pairs, width)) + bias
    cot_p[...] = mm(pair_perm, cot_v[...].reshape(pairs, width)).astype(BF16)
    back_v[...] = mm(cot_p[...], down_v[...], NT)

    for d in range(1, ncol):
        src = col_peer(d)
        landed(a_buf.at[src], a_recv_sem.at[src])
    a_all = a_buf[...].reshape(seqs, rows * C)
    a_p[...] = mm(a_all, permt_v[...]).astype(BF16)
    a_pt[...] = (mm(perm_v[...], a_all, NT) * scale).astype(BF16)

    part = CHUNK // C * rows
    tiles = CHUNK // LANES
    blocks = C // QUARTERS
    def chunk(k, carry):
        for d in range(1, nrow):
            src = row_peer(d)
            landed(b_buf.at[k, src], b_recv_sem.at[k, src])
        b_k = b_buf[k].reshape(seqs, CHUNK)
        m = mm(a_pt[...], b_k)
        for t in range(tiles):
            for h in range(blocks):
                r = quarter_transpose(
                    [
                        m[(h * QUARTERS + q) * rows:(h * QUARTERS + q + 1) * rows, t * LANES:(t + 1) * LANES]
                        for q in range(QUARTERS)
                    ]
                )
                for q in range(QUARTERS):
                    j = t * QUARTERS + q
                    o_v[j * rows:(j + 1) * rows, h * LANES:(h + 1) * LANES] = r[q].astype(BF16)
        span = pl.ds(pl.multiple_of(k * part, part), part)
        middle = pin_p[span, :] + mm(o_v[...], w_v[...])
        centred = middle - jnp.mean(middle, axis=-1, keepdims=True)
        inverse = lax.rsqrt(jnp.mean(centred * centred, axis=-1, keepdims=True) + 1e-05)
        xhat = centred * inverse
        normed = (xhat * gain).astype(BF16)
        preact = mm(normed, up_v[...])
        hidden = jnp.maximum(preact, 0.0).astype(BF16)
        hid_v[span, :] = hidden
        pin_p[span, :] = middle
        d_hidden = jnp.where(preact > 0.0, back_v[span, :], 0.0).astype(BF16)
        d_normed = mm(d_hidden, up_v[...], NT)
        scaled = d_normed * gain
        d_middle = cot_p[span, :].astype(F32) + inverse * (
            scaled
            - jnp.mean(scaled, axis=-1, keepdims=True)
            - xhat * jnp.mean(scaled * xhat, axis=-1, keepdims=True)
        )
        d_outer = mm(d_middle.astype(BF16), w_v[...], NT)
        for t in range(tiles):
            for h in range(blocks):
                r = quarter_transpose(
                    [
                        d_outer[(t * QUARTERS + q) * rows:(t * QUARTERS + q + 1) * rows, h * LANES:(h + 1) * LANES]
                        for q in range(QUARTERS)
                    ]
                )
                for q in range(QUARTERS):
                    c = h * QUARTERS + q
                    d_v[c * rows:(c + 1) * rows, t * LANES:(t + 1) * LANES] = r[q].astype(BF16)
        gr_send[k] = mm(a_p[...], d_v[...]).astype(BF16).reshape(gr_send.shape[1:])
        for d in range(1, nrow):
            gr_copy(k, d).start()
        gl = mm(b_k, d_v[...], NT)
        gl_acc[...] += gl
        return carry

    gl_acc[...] = jnp.zeros_like(gl_acc)
    lax.fori_loop(0, nch, chunk, 0)
    gl_send[...] = gl_acc[...].astype(BF16).reshape(gl_send.shape)
    for d in range(1, ncol):
        go(gl_copy(d))

    out_p = (pin_p[...] + mm(hid_v[...], down_v[...])).astype(BF16)
    out_ref[...] = mm(pair_permt, out_p).astype(BF16).reshape(out_ref.shape)

    for k in range(nch):
        total = gr_send[k, me_r].astype(F32)
        for d in range(1, nrow):
            src = row_peer(d)
            landed(gr_recv.at[k, src], gr_recv_sem.at[k, src])
            total = total + gr_recv[k, src].astype(F32)
        gr_ref[:, k * CHUNK:(k + 1) * CHUNK] = (total * scale).astype(BF16)
    total = gl_send[me_c].astype(F32)
    for d in range(1, ncol):
        src = col_peer(d)
        landed(gl_recv.at[src], gl_recv_sem.at[src])
        total = total + gl_recv[src].astype(F32)
    gl_ref[...] = mm((total * scale).astype(BF16), perm_v[...]).astype(BF16)
    for copy in sends:
        copy.wait_send()
    for k in range(nch):
        for d in range(1, nrow):
            gr_copy(k, d).wait_send()


def put_out(a, b, c, x, y, z, sem):
    copies = [pltpu.make_async_copy(s, t, sem.at[n]) for n, (s, t) in enumerate([(a, x), (b, y), (c, z)])]
    for copy in copies:
        copy.start()
    for copy in copies:
        copy.wait()


def on_device(nrow, ncol, left, right, pair_in, pair_cot, ln_gain, out_weight, out_bias, trans_up, trans_down):
    rows, cols, width = pair_in.shape
    ls, lw = left.shape
    rs, rw = right.shape
    seqs = ls * ncol
    ffn = trans_up.shape[1]
    pairs = rows * cols
    nch = rw // CHUNK
    dma = pltpu.SemaphoreType.DMA
    vm = pltpu.VMEM
    scratch = [
        vm((ls, lw), BF16), vm((rs, rw), BF16),
        vm((rows, cols, width), BF16), vm((rows, cols, width), BF16),
        vm(out_weight.shape, BF16), vm(trans_up.shape, BF16), vm(trans_down.shape, BF16),
        vm(ln_gain.shape, F32), vm(out_bias.shape, F32),
        vm((ncol, ls, lw), BF16), vm((nch, nrow, rs, CHUNK), BF16),
        vm((lw, lw), BF16), vm((lw, lw), BF16),
        vm((pairs, width), F32), vm((pairs, width), BF16), vm((pairs, ffn), F32),
        vm((seqs, lw), BF16), vm((lw, seqs), BF16),
        vm((CHUNK // C * rows, C * C), BF16), vm((pairs, ffn), BF16), vm((lw, CHUNK), BF16),
        vm((nch, nrow, rs, CHUNK), BF16), vm((nch, nrow, rs, CHUNK), BF16),
        vm((seqs, lw), F32), vm((ncol, ls, lw), BF16), vm((ncol, ls, lw), BF16),
        dma((9,)), dma((ncol,)), dma((ncol,)), dma((nch, nrow)), dma((nch, nrow)),
        dma((nch, nrow)), dma((nch, nrow)), dma((ncol,)), dma((ncol,)),
    ]
    hbm = pl.BlockSpec(memory_space=pltpu.HBM)
    vmem = pl.BlockSpec(memory_space=pltpu.VMEM)
    results = pl.pallas_call(
        functools.partial(kernel, nrow, ncol, rows, cols),
        out_shape=(
            pltpu.VMEM(pair_in.shape, BF16),
            pltpu.VMEM(left.shape, BF16),
            pltpu.VMEM(right.shape, BF16),
        ),
        in_specs=[hbm] * 9,
        out_specs=(vmem, vmem, vmem),
        scratch_shapes=scratch,
        compiler_params=pltpu.CompilerParams(collective_id=0, has_side_effects=True),
    )(left, right, pair_in, pair_cot, ln_gain, out_weight, out_bias, trans_up, trans_down)
    return pl.pallas_call(
        put_out,
        out_shape=tuple(jax.ShapeDtypeStruct(x.shape, x.dtype) for x in results),
        in_specs=[vmem] * 3,
        out_specs=(hbm, hbm, hbm),
        scratch_shapes=[dma((3,))],
        compiler_params=pltpu.CompilerParams(vmem_limit_bytes=LIMIT // 8),
    )(*results)


def solution(mesh):
    nrow, ncol = mesh.shape["row"], mesh.shape["col"]
    return jax.shard_map(
        functools.partial(on_device, nrow, ncol),
        mesh=mesh,
        in_specs=(
            P("col", "row"),
            P("row", "col"),
            P("row", "col", None),
            P("row", "col", None),
            P(),
            P(),
            P(),
            P(),
            P(),
        ),
        out_specs=(P("row", "col", None), P("col", "row"), P("row", "col")),
        check_vma=False,
    )
```
